32 devices in a mesh: cuts: 4 (over z), fsdp: 8 (over y, x, core).
Axes of the slice: x: 2, y: 2, z: 4, core: 2. Of those that a mesh axis runs over, the one named last changes fastest.
Arguments:
- tokens: bfloat16 [4096, 8192], P(('cuts', 'fsdp')), may hold values from -240 to 240
- norm_gain: bfloat16 [8192], P('fsdp'), may hold values from 0.5 to 1.5
- gate_weight: bfloat16 [8192, 256], P('fsdp'), may hold values from -0.0625 to 0.0625
- up_weight: bfloat16 [8192, 256], P('fsdp'), may hold values from -0.0625 to 0.0625
- down_weight: bfloat16 [256, 8192], P(None, 'fsdp'), may hold values from -0.375 to 0.375
- slice_grads: float32 [4, 3, 8192, 256], P('cuts', None, 'fsdp'), may hold values from -6 to 6
Outputs:
- branch_out: bfloat16 [4096, 8192], P(('cuts', 'fsdp'))
- grad_mean: float32 [3, 8192, 256], P(None, 'fsdp')
The draws below stay inside these ranges and needn't reach their ends.
All inputs are finite; a program needn't handle non-finite values.
Results may differ from the reference program's by a relative error of at most 0.0065.
Values may be sent and summed in bfloat16 or wider, within the bound.
A program may use at most 64 MiB of HBM per device.

```python
import math
import jax
import jax.numpy as jnp
from jax import lax

D = 8192
F = 256
TOK_DEV = 128
TOKENS = 4096
N_CUTS = 4


def draw_tokens(key, part):
    key_base = jax.random.fold_in(key, 11)
    key_rows = jax.random.fold_in(key, 12)
    key_cols = jax.random.fold_in(key, 13)
    base_draw = jax.random.normal(key_base, (TOKENS, D), jnp.float32)
    base_draw = jnp.clip(base_draw, -6.0, 6.0)
    row_scale = jnp.exp(jax.random.uniform(key_rows, (TOKENS, 1), jnp.float32, 0.0, math.log(10.0)))
    col_scale = jnp.exp(jax.random.uniform(key_cols, (1, D), jnp.float32, math.log(0.4), math.log(4.0)))
    return (base_draw * row_scale * col_scale).astype(jnp.bfloat16)


def levels(own_key, extent, cuts, low, high):
    def one(position, blocks):
        draws = jax.random.uniform(jax.random.fold_in(jax.random.fold_in(own_key, 6), position), (blocks,), jnp.float32, low / len(cuts), high / len(cuts))
        return jnp.repeat(jnp.exp(draws), extent[position] // blocks).reshape((-1,) + (1,) * (len(extent) - position - 1))

    loudness = one(*cuts[0])
    for cut in cuts[1:]:
        loudness = loudness * one(*cut)
    return loudness


def gaussian(key, shape, width, most, cuts=(), held_as=jnp.bfloat16):
    loudness = levels(key, shape, cuts, -0.22, 0.18) if cuts else 1.0
    values = jax.random.normal(key, shape, jnp.float32) * width * loudness
    return jnp.minimum(jnp.maximum(values, -most), most).astype(held_as)


def setup_inputs(seed: int = 0) -> dict:
    key_list = jax.random.split(jax.random.key(seed), 7)
    tokens = draw_tokens(jax.random.fold_in(key_list[6], 71), 0)
    norm_gain = jnp.clip(1.0 + 0.1 * jax.random.normal(key_list[1], (D,), jnp.float32), 0.5, 1.5).astype(jnp.bfloat16)
    gate_weight = gaussian(key_list[2], (D, F), D ** -0.5, 0.0625, ((0, 8),))
    up_weight = gaussian(key_list[3], (D, F), D ** -0.5, 0.0625, ((0, 8),))
    down_weight = gaussian(key_list[4], (F, D), F ** -0.5, 0.375, ((1, 8),))
    slice_grads = gaussian(key_list[5], (N_CUTS, 3, D, F), 1.0, 6.0, ((0, 4), (2, 8)), jnp.float32)
    return {"tokens": tokens, "norm_gain": norm_gain, "gate_weight": gate_weight, "up_weight": up_weight, "down_weight": down_weight, "slice_grads": slice_grads}


def feed_block(token_block, norm_gain, gate_weight, up_weight, down_weight):
    tok_float = token_block.astype(jnp.float32)
    inv_rms = lax.rsqrt(lax.optimization_barrier(jnp.mean(tok_float * tok_float, axis=1, keepdims=True)) + 1e-05)
    normed = (tok_float * inv_rms * norm_gain.astype(jnp.float32)[None, :]).astype(jnp.bfloat16)
    gate_out = jnp.dot(normed, gate_weight, preferred_element_type=jnp.float32)
    up_out = jnp.dot(normed, up_weight, preferred_element_type=jnp.float32)
    hidden = (jax.nn.silu(gate_out) * up_out).astype(jnp.bfloat16)
    return jnp.dot(hidden, down_weight, preferred_element_type=jnp.float32).astype(jnp.bfloat16)

def reference(tokens, norm_gain, gate_weight, up_weight, down_weight, slice_grads):
    block_rows = 4 * TOK_DEV
    blocked = tokens.reshape(TOKENS // block_rows, block_rows, D)

    def one_block(token_block):
        return feed_block(token_block, norm_gain, gate_weight, up_weight, down_weight)
    branch_out = lax.map(one_block, blocked).reshape(TOKENS, D)
    grad_mean = lax.optimization_barrier(jnp.sum(slice_grads, axis=0)) / N_CUTS
    return (branch_out, grad_mean)
```

```python
import functools

import jax
import jax.numpy as jnp
from jax import lax
from jax.experimental import pallas as pl
from jax.experimental.pallas import tpu as pltpu
from jax.sharding import PartitionSpec as P

MESH = pl.DeviceIdType.MESH
F32, BF16 = jnp.float32, jnp.bfloat16
CORES = 2
AHEAD = 2
ROW_PIECES = 8
K_BLOCKS = 2
GRAD_CHUNKS = 8
LANES = 128
ROWS = 16


def gray(pos, count):
    chip, bit = 0, 1
    while bit < count:
        chip = chip + bit * ((pos // bit + pos // (2 * bit)) % 2)
        bit *= 2
    return chip


def ungray(chip, count):
    pos, bit = 0, 1
    while bit < count:
        above, high = 0, bit
        while high < count:
            above = above + (chip // high) % 2
            high *= 2
        pos = pos + bit * (above % 2)
        bit *= 2
    return pos


def kernel(
    n, nc, tok_hbm, gain_ref, gate_hbm, up_hbm, down_hbm, grad_hbm, out_ref, mean_ref,
    wgu, wd, tok, gains, own_grad, rbuf, sbuf, tbuf, acc, hid, inv,
    load_sem, gain_send, gain_recv, link_send, pair_send, piece_recv,
    red_send, red_recv, tot_send, tot_recv,
):
    chips = n // CORES
    half_ring = chips // 2
    depth, width = gate_hbm.shape
    half = depth // 2
    row_piece = half // ROW_PIECES
    col_pieces = half // LANES
    pieces = ROW_PIECES + col_pieces
    k_block = half // K_BLOCKS

    me = lax.axis_index("fsdp")
    z = lax.axis_index("cuts")
    chip, core = me // CORES, me % CORES
    other = 1 - core
    partner = chip * CORES + other
    pos = ungray(chip, chips)

    def device(offset, which):
        return gray((pos + offset + chips) % chips, chips) * CORES + which

    right, left = device(1, core), device(-1, core)

    loads = [
        pltpu.make_async_copy(gate_hbm, wgu.at[me, :, pl.ds(0, width)], load_sem.at[0]),
        pltpu.make_async_copy(up_hbm, wgu.at[me, :, pl.ds(width, width)], load_sem.at[1]),
        pltpu.make_async_copy(down_hbm, wd.at[me], load_sem.at[2]),
        pltpu.make_async_copy(grad_hbm, own_grad, load_sem.at[3]),
        pltpu.make_async_copy(tok_hbm, tok, load_sem.at[4]),
    ]
    for load in loads:
        load.start()
    gains[me] = gain_ref[...].astype(F32)

    barrier = pltpu.get_barrier_semaphore()
    for step in range(1, n):
        pl.semaphore_signal(barrier, inc=1, device_id={"fsdp": (me + step) % n}, device_id_type=MESH)

    for step in (1, nc - 1):
        pl.semaphore_signal(barrier, inc=1, device_id={"cuts": (z + step) % nc}, device_id_type=MESH)
    pl.semaphore_wait(barrier, n + 1)

    def remote(src, dst, send, recv, to):
        return pltpu.make_async_remote_copy(
            src_ref=src, dst_ref=dst, send_sem=send, recv_sem=recv, device_id=to, device_id_type=MESH
        )

    def piece(origin, h, i):
        if i < ROW_PIECES:
            return wgu.at[origin, pl.ds(h * half + i * row_piece, row_piece), :]
        return wd.at[origin, :, pl.ds(h * half + (i - ROW_PIECES) * LANES, LANES)]

    def move(origin, h, i, send, to):
        ref = piece(origin, h, i)
        return remote(ref, ref, send, piece_recv.at[origin, h, i], {"fsdp": to})

    def halves(way, distance):
        both = (0, 1) if way == 0 else (1, 0)
        return both if distance < half_ring else both[:1]

    sent = []

    def link(way, distance, origin, h, i):
        copy = move(origin, h, i, link_send.at[way, distance - 1, h, i], right if way == 0 else left)
        copy.start()
        sent.append(copy)

    def pair(chip_offset, origin, h, i):
        copy = move(origin, h, i, pair_send.at[chip_offset % chips, h, i], partner)
        copy.start()
        sent.append(copy)

    def send_own(i):
        for turn in range(2):
            for way in range(2):
                order = halves(way, 1)
                if turn < len(order):
                    link(way, 1, me, order[turn], i)
        for h in range(2):
            pair(0, me, h, i)

    loads[0].wait()
    loads[1].wait()
    for i in range(AHEAD):
        send_own(i)
    gain_copies = []
    for step in range(1, n):
        copy = remote(
            gains.at[me], gains.at[me], gain_send.at[step], gain_recv.at[step], {"fsdp": (me + step) % n}
        )
        copy.start()
        gain_copies.append(copy)
    loads[2].wait()
    loads[3].wait()

    rows = own_grad.shape[0] // (2 * GRAD_CHUNKS)
    roots = ((nc - 1) // 2, nc // 2)

    def grad_tick(t):
        for g, root in enumerate(roots):
            deepest = max(root, nc - 1 - root)
            on_left = z < root
            side = jnp.where(on_left, 0, 1)
            inner = jnp.where(on_left, z + 1, z - 1)
            outer = jnp.where(on_left, z - 1, z + 1)
            outermost = jnp.where(on_left, z == 0, z == nc - 1)

            def span(j):
                return pl.ds(pl.multiple_of((g * GRAD_CHUNKS + j) * rows, rows), rows)

            def red(j, s, to):
                return remote(
                    sbuf.at[span(j), :], rbuf.at[s, span(j), :],
                    red_send.at[g, j], red_recv.at[s, g, j], {"cuts": to},
                )

            def tot(j, s, to):
                return remote(
                    tbuf.at[span(j), :], tbuf.at[span(j), :], tot_send.at[s, g, j], tot_recv.at[g, j], {"cuts": to}
                )

            j = t - jnp.where(on_left, z, nc - 1 - z)

            @pl.when((z != root) & (j >= 0) & (j < GRAD_CHUNKS))
            def _():
                @pl.when(outermost)
                def _():
                    sbuf[span(j), :] = own_grad[span(j), :].astype(BF16)

                @pl.when(jnp.logical_not(outermost))
                def _():
                    red(j, side, inner).wait_recv()
                    sbuf[span(j), :] = (own_grad[span(j), :] + rbuf[side, span(j), :].astype(F32)).astype(BF16)

                red(j, side, inner).start()

            jm = t - deepest
            if 0 <= jm < GRAD_CHUNKS:

                @pl.when(z == root)
                def _():
                    total = own_grad[span(jm), :]
                    if root > 0:
                        red(jm, 0, z - 1).wait_recv()
                        total = total + rbuf[0, span(jm), :].astype(F32)
                    if root < nc - 1:
                        red(jm, 1, z + 1).wait_recv()
                        total = total + rbuf[1, span(jm), :].astype(F32)
                    mean = (total / nc).astype(BF16)
                    tbuf[span(jm), :] = mean
                    mean_ref[span(jm), :] = mean.astype(F32)
                    if root > 0:
                        tot(jm, 0, z - 1).start()
                    if root < nc - 1:
                        tot(jm, 1, z + 1).start()

            jb = t - deepest - jnp.where(on_left, root - z, z - root)

            @pl.when((z != root) & (jb >= 0) & (jb < GRAD_CHUNKS))
            def _():
                tot(jb, side, inner).wait_recv()

                @pl.when(jnp.logical_not(outermost))
                def _():
                    tot(jb, side, outer).start()

                mean_ref[span(jb), :] = tbuf[span(jb), :].astype(F32)

    def grad_end():
        for g, root in enumerate(roots):
            for j in range(GRAD_CHUNKS):
                at = pl.ds((g * GRAD_CHUNKS + j) * rows, rows)
                on_left = z < root
                side = jnp.where(on_left, 0, 1)
                outermost = jnp.where(on_left, z == 0, z == nc - 1)

                def wait(sem, to):
                    remote(sbuf.at[at, :], tbuf.at[at, :], sem, tot_recv.at[g, j], {"cuts": to}).wait_send()

                @pl.when(z != root)
                def _():
                    wait(red_send.at[g, j], jnp.where(on_left, z + 1, z - 1))

                    @pl.when(jnp.logical_not(outermost))
                    def _():
                        wait(tot_send.at[side, g, j], jnp.where(on_left, z - 1, z + 1))

                @pl.when(z == root)
                def _():
                    if root > 0:
                        wait(tot_send.at[0, g, j], z - 1)
                    if root < nc - 1:
                        wait(tot_send.at[1, g, j], z + 1)

    def ring_tick(t):
        if AHEAD <= t + AHEAD < pieces:
            send_own(t + AHEAD)
        for distance in range(1, half_ring + 1):
            i = t - (distance - 1)
            if not 0 <= i < pieces:
                continue
            for turn in range(2):
                for way in range(2):
                    order = halves(way, distance)
                    if turn >= len(order):
                        continue
                    h = order[turn]
                    offset = -distance if way == 0 else distance
                    origin = device(offset, core)
                    move(origin, h, i, link_send.at[way, 0, h, i], right).wait_recv()
                    if distance < half_ring and h in halves(way, distance + 1):
                        link(way, distance + 1, origin, h, i)
                    pair(offset, origin, h, i)

    def wait_partner(lo, hi):
        def one(c, _):
            origin = c * CORES + other
            for i in range(lo, hi):
                for h in range(2):
                    move(origin, h, i, pair_send.at[0, h, i], partner).wait_recv()
            return 0

        lax.fori_loop(0, chips, one, 0)

    def gate_up(which, b):
        def one(c, _):
            origin = c * CORES + which
            for h in range(2):
                first = h * half + b * k_block
                at = pl.ds(pl.multiple_of(origin * depth + first, LANES), k_block)
                scaled = tok[:, at].astype(F32) * inv[...] * gains[origin, :, pl.ds(first, k_block)]
                acc[...] += jnp.dot(
                    scaled.astype(BF16), wgu[origin, pl.ds(first, k_block), :], preferred_element_type=F32
                )
            return 0

        lax.fori_loop(0, chips, one, 0)

    def down(which, i):
        def one(c, _):
            origin = c * CORES + which
            for h in range(2):
                first = h * half + (i - ROW_PIECES) * LANES
                at = pl.ds(pl.multiple_of(origin * depth + first, LANES), LANES)
                out_ref[:, at] = jnp.dot(
                    hid[...], wd[origin, :, pl.ds(first, LANES)], preferred_element_type=F32
                ).astype(BF16)
            return 0

        lax.fori_loop(0, chips, one, 0)

    def norms():
        loads[4].wait()
        total = jnp.zeros((tok.shape[0], 1), F32)

        def one(c, total):
            part = tok[:, pl.ds(pl.multiple_of(c * depth, LANES), depth)].astype(F32)
            return total + jnp.sum(part * part, axis=1, keepdims=True)

        total = lax.fori_loop(0, n, one, total)
        inv[...] = lax.rsqrt(total / tok.shape[1] + 1e-05)
        acc[...] = jnp.zeros_like(acc)

    def finish_hidden():
        gate, up = acc[:, :width], acc[:, width:]
        hid[...] = (gate / (1.0 + jnp.exp(-gate)) * up).astype(BF16)

    work = {}

    def at_tick(t, job):
        work.setdefault(t, []).append(job)

    at_tick(0, norms)
    ready = 0
    for b in range(K_BLOCKS):
        lo, hi = b * ROW_PIECES // K_BLOCKS, (b + 1) * ROW_PIECES // K_BLOCKS
        own_tick, pair_tick = hi - 1 + half_ring - 1, hi - 1 + half_ring
        if b == 0:

            def gains_here():
                for copy in gain_copies:
                    copy.wait_recv()

            at_tick(own_tick, gains_here)
        at_tick(own_tick, functools.partial(gate_up, core, b))
        at_tick(pair_tick, functools.partial(wait_partner, lo, hi))
        at_tick(pair_tick, functools.partial(gate_up, other, b))
        ready = pair_tick
    at_tick(ready, finish_hidden)
    for i in range(ROW_PIECES, pieces):
        at_tick(max(ready + 1, i + half_ring - 1), functools.partial(down, core, i))
        pair_tick = max(ready + 1, i + half_ring)
        at_tick(pair_tick, functools.partial(wait_partner, i, i + 1))
        at_tick(pair_tick, functools.partial(down, other, i))
    farthest = max(max(r, nc - 1 - r) for r in roots)
    ticks = max(max(work) + 1, GRAD_CHUNKS + 2 * farthest)
    for t in range(ticks):
        ring_tick(t)
        grad_tick(t)
        for job in work.get(t, ()):
            job()

    for copy in sent + gain_copies:
        copy.wait_send()
    grad_end()


def fits(n, nc, depth, width, grad_rows):
    chips = n // CORES
    ring = n % CORES == 0 and chips >= 2 and chips & (chips - 1) == 0
    whole = depth % (2 * LANES * K_BLOCKS) == 0 and depth % (2 * ROW_PIECES * ROWS) == 0
    return ring and nc > 1 and whole and width % LANES == 0 and grad_rows % (2 * GRAD_CHUNKS * ROWS) == 0


def plain(tokens, norm_gain, gate_weight, up_weight, down_weight, slice_grads):
    tok = tokens.astype(F32)
    inv = lax.rsqrt(jnp.mean(tok * tok, axis=1, keepdims=True) + 1e-05)
    gate_full, up_full, gain = (
        lax.all_gather(part, "fsdp", axis=0, tiled=True) for part in (gate_weight, up_weight, norm_gain)
    )
    normed = (tok * inv * gain.astype(F32)[None, :]).astype(BF16)
    gate = jnp.dot(normed, gate_full, preferred_element_type=F32)
    up = jnp.dot(normed, up_full, preferred_element_type=F32)
    hidden = (jax.nn.silu(gate) * up).astype(BF16)
    down_full = lax.all_gather(down_weight, "fsdp", axis=1, tiled=True)
    branch = jnp.dot(hidden, down_full, preferred_element_type=F32).astype(BF16)
    return branch, lax.psum(slice_grads[0], "cuts") / lax.axis_size("cuts")


def solution(mesh):
    n, nc = mesh.shape["fsdp"], mesh.shape["cuts"]

    def per_device(tokens, norm_gain, gate_weight, up_weight, down_weight, slice_grads):
        depth, width = gate_weight.shape
        grads = slice_grads.reshape(-1, slice_grads.shape[-1])
        if not fits(n, nc, depth, width, grads.shape[0]):
            return plain(tokens, norm_gain, gate_weight, up_weight, down_weight, slice_grads)
        chips = n // CORES
        pieces = ROW_PIECES + depth // 2 // LANES
        hbm, vmem = pl.BlockSpec(memory_space=pl.ANY), pl.BlockSpec(memory_space=pltpu.VMEM)
        dma = pltpu.SemaphoreType.DMA
        branch, mean = pl.pallas_call(
            functools.partial(kernel, n, nc),
            out_shape=(
                jax.ShapeDtypeStruct(tokens.shape, BF16),
                jax.ShapeDtypeStruct(grads.shape, F32),
            ),
            in_specs=[hbm, vmem, hbm, hbm, hbm, hbm],
            out_specs=(vmem, vmem),
            scratch_shapes=[
                pltpu.VMEM((n, depth, 2 * width), BF16),
                pltpu.VMEM((n, width, depth), BF16),
                pltpu.VMEM(tokens.shape, BF16),
                pltpu.VMEM((n, 1, depth), F32),
                pltpu.VMEM(grads.shape, F32),
                pltpu.VMEM((2,) + grads.shape, BF16),
                pltpu.VMEM(grads.shape, BF16),
                pltpu.VMEM(grads.shape, BF16),
                pltpu.VMEM((tokens.shape[0], 2 * width), F32),
                pltpu.VMEM((tokens.shape[0], width), BF16),
                pltpu.VMEM((tokens.shape[0], 1), F32),
                dma((5,)),
                dma((n,)),
                dma((n,)),
                dma((2, chips // 2, 2, pieces)),
                dma((chips, 2, pieces)),
                dma((n, 2, pieces)),
                dma((2, GRAD_CHUNKS)),
                dma((2, 2, GRAD_CHUNKS)),
                dma((2, 2, GRAD_CHUNKS)),
                dma((2, GRAD_CHUNKS)),
            ],
            compiler_params=pltpu.CompilerParams(collective_id=0, has_side_effects=True),
        )(tokens, norm_gain.reshape(1, -1), gate_weight, up_weight, down_weight, grads)
        return branch, mean.reshape(slice_grads.shape[1:])

    return jax.shard_map(
        per_device,
        mesh=mesh,
        in_specs=(
            P(("cuts", "fsdp"), None),
            P("fsdp"),
            P("fsdp", None),
            P("fsdp", None),
            P(None, "fsdp"),
            P("cuts", None, "fsdp", None),
        ),
        out_specs=(P(("cuts", "fsdp"), None), P(None, "fsdp", None)),
        check_vma=False,
    )
```
